512 devices in a mesh: cells: 32 (over x, y, core), vocab: 16 (over z).
Axes of the slice: x: 4, y: 4, z: 16, core: 2. Of those that a mesh axis runs over, the one named last changes fastest.
Arguments:
- clean_resid: float32 [32, 2048], P('cells'), may hold values from -130 to 130
- path_delta: bfloat16 [32, 4, 16, 2048], P('cells'), may hold values from -6 to 6
- layer_index: int32 [4064], P('cells'), may hold values from 0 to 3
- pos_index: int32 [4064], P('cells'), may hold values from 0 to 15
- answer_ids: int32 [32], P('cells'), may hold values from 0 to 51199
- norm_gain: float32 [2048], replicated, may hold values from 0.1 to 1.9
- unembed: bfloat16 [2048, 51200], P('cells', 'vocab'), may hold values from -1.5 to 1.5
Outputs:
- divergence: float32 [4064], P('cells')
- answer_logprob: float32 [4064], P('cells')
- total_kl: float32 [], replicated
The draws below stay inside these ranges and needn't reach their ends.
All inputs are finite; a program needn't handle non-finite values.
Results may differ from the reference program's by a relative error of at most 0.0091.
Values may be sent and summed in bfloat16 or wider, within the bound.
No kernel may reach another device: no remote copies, remote signals or barrier semaphores. Data moves between devices by JAX's collectives and lax.ppermute only.
A program may use at most 64 MiB of HBM per device.

```python
import math
import jax
import jax.numpy as jnp
from jax import lax

D = 2048
VOCAB = 51200
LAYERS = 4
POS = 16
PROMPTS = 32
CELLS = 4064


def draw_unembed(key, part):
    values = jnp.clip(jax.random.normal(jax.random.fold_in(key, 202), (D, VOCAB), jnp.float32), -6.0, 6.0) / math.sqrt(D)
    return values.astype(jnp.bfloat16)


def draw_clean_resid(key, part):
    values = jnp.clip(jax.random.normal(jax.random.fold_in(key, 303), (PROMPTS, D), jnp.float32), -6.0, 6.0)
    return values


def with_ends(result, stream_key, least, high):
    shape = result.shape
    index_at = [jax.random.randint(jax.random.fold_in(stream_key, axis), (), 0, shape[axis]) for axis in range(len(shape))]
    result = result.at[tuple(index_at)].set(least)
    longest = shape.index(max(shape))
    index_at[longest] = (index_at[longest] + 1) % shape[longest]
    return result.at[tuple(index_at)].set(high)


def steps_of(rng, dims, shards, smallest, high):
    loudness, own = 1.0, jax.random.fold_in(rng, 6)
    for dim, shards_of in shards:
        steps = jnp.exp(jax.random.uniform(jax.random.fold_in(own, dim), (shards_of,), jnp.float32, smallest / len(shards), high / len(shards)))
        loudness = loudness * jnp.repeat(steps, dims[dim] // shards_of).reshape([-1 if axis == dim else 1 for axis in range(len(dims))])
    return loudness


def noise(key, dims, scale, most, shards=(), held_as=jnp.bfloat16):
    drawn = jax.random.normal(key, dims, jnp.float32) * scale
    if len(shards) > 0:
        drawn = steps_of(key, dims, shards, -0.22, 0.18) * drawn
    return jnp.clip(drawn, min=-most, max=most).astype(held_as)


def setup_inputs(seed: int = 0) -> dict:
    seeds = jax.random.split(jax.random.key(seed), 8)
    return {
        "clean_resid": draw_clean_resid(jax.random.fold_in(seeds[7], 71), 0),
        "path_delta": noise(seeds[1], (PROMPTS, LAYERS, POS, D), 1.0, 6.0, ((0, 32),)),
        "layer_index": with_ends(jax.random.randint(seeds[2], (CELLS,), 0, LAYERS), jax.random.fold_in(seeds[2], 1), 0, LAYERS - 1).astype(jnp.int32),
        "pos_index": with_ends(jax.random.randint(seeds[3], (CELLS,), 0, POS), jax.random.fold_in(seeds[3], 1), 0, POS - 1).astype(jnp.int32),
        "answer_ids": with_ends(jax.random.randint(seeds[4], (PROMPTS,), 0, VOCAB), jax.random.fold_in(seeds[4], 1), 0, VOCAB - 1).astype(jnp.int32),
        "norm_gain": jnp.clip(1.0 + 0.18 * jax.random.normal(seeds[5], (D,), jnp.float32), 0.1, 1.9),
        "unembed": draw_unembed(jax.random.fold_in(seeds[7], 71), 0),
    }


def normalize_rows(values, norm_gain):
    mean_square = lax.optimization_barrier(jnp.mean(values * values, axis=-1, keepdims=True))
    return (values * lax.rsqrt(mean_square + 1e-06) * norm_gain).astype(jnp.bfloat16)

def reference(clean_resid, path_delta, layer_index, pos_index, answer_ids, norm_gain, unembed):
    prompt_count = clean_resid.shape[0]
    cell_count = layer_index.shape[0]
    per_prompt = cell_count // prompt_count
    owner_prompt = (jnp.arange(cell_count, dtype=jnp.int32) // per_prompt).astype(jnp.int32)
    delta_rows = path_delta[owner_prompt, layer_index, pos_index].astype(jnp.float32)
    patched_resid = clean_resid[owner_prompt] + delta_rows
    clean_normed = normalize_rows(clean_resid, norm_gain)
    patched_normed = normalize_rows(patched_resid, norm_gain).reshape(prompt_count, per_prompt, -1)
    weight_full = unembed.astype(jnp.float32)

    def score_prompt(inputs):
        clean_row, patched_rows, answer = inputs
        clean_logits = jnp.dot(clean_row.astype(jnp.float32)[None, :], weight_full, precision=lax.Precision.HIGHEST)[0]
        patched_logits = jnp.dot(patched_rows.astype(jnp.float32), weight_full, precision=lax.Precision.HIGHEST)
        clean_lse = jax.nn.logsumexp(clean_logits)
        patched_lse = jax.nn.logsumexp(patched_logits, axis=-1)
        clean_prob = jnp.exp(clean_logits - clean_lse)
        divergence = lax.optimization_barrier(jnp.sum(clean_prob[None, :] * (clean_logits[None, :] - patched_logits), axis=-1)) - clean_lse + patched_lse
        answer_logit = lax.dynamic_index_in_dim(patched_logits, answer, 1, keepdims=False)
        return (divergence, answer_logit - patched_lse)
    divergence, answer_logprob = lax.map(score_prompt, (clean_normed, patched_normed, answer_ids))
    divergence = divergence.reshape(-1)
    return (divergence, answer_logprob.reshape(-1), jnp.sum(divergence))
```

```python
import jax
import jax.numpy as jnp
from jax import lax
from jax.experimental import pallas as pl
from jax.experimental.pallas import tpu as pltpu
from jax.sharding import PartitionSpec as P

XS, YS, CORES = 4, 4, 2
SUBS = YS * CORES
PLANE = XS * SUBS
LANES = 128
KEYS = 64
ROWS = 80
FULL = 3
LEFT = LANES // SUBS
NEG = -1e30
F32 = jnp.float32
BF16 = jnp.bfloat16
VMEM = pl.BlockSpec(memory_space=pltpu.VMEM)
SMEM = pl.BlockSpec(memory_space=pltpu.SMEM)


def lanes_of(shape):
    return lax.broadcasted_iota(jnp.int32, shape, len(shape) - 1)


def pack_kernel(u_ref, out_ref):
    depth = u_ref.shape[0]
    groups = depth // 8
    last = u_ref[:, SUBS * FULL * LANES :].astype(F32)
    lane = lanes_of((8, LANES))
    for sub in range(SUBS):
        left = jnp.zeros((8, LANES), F32)
        for a in range(groups):
            piece = pltpu.roll(last[8 * a : 8 * a + 8], (LEFT * (a - sub)) % LANES, 1)
            left = jnp.where(lane // LEFT == a, piece, left)
        left = left.astype(BF16)
        for x in range(XS):
            to = x * SUBS + sub
            for k in range(FULL):
                at = (sub * FULL + k) * LANES
                out_ref[to, k * depth : (k + 1) * depth, :] = u_ref[:, at : at + LANES]
            out_ref[to, FULL * depth :, :] = left


def packed(unembed):
    depth = unembed.shape[0]
    return pl.pallas_call(
        pack_kernel,
        out_shape=jax.ShapeDtypeStruct((PLANE, FULL * depth + 8, LANES), BF16),
        in_specs=[VMEM],
        out_specs=VMEM,
        name="pack",
    )(unembed)


def norm_kernel(answer_ref, clean_ref, delta_ref, gain_ref, flat_ref, act_ref, count_ref):
    features = clean_ref.shape[1]
    clean = clean_ref[...]
    gain = gain_ref[...]

    def normed(values):
        mean_square = jnp.sum(values * values, axis=-1, keepdims=True) * (1.0 / features)
        return values * lax.rsqrt(mean_square + 1e-06) * gain

    act_ref[:KEYS, :] = normed(clean + delta_ref[...].astype(F32)).astype(BF16)
    answer = answer_ref[0]
    high = lax.shift_right_logical(answer, 8).astype(F32)
    low = (answer & 255).astype(F32)
    shape = (ROWS - KEYS, features)
    row = lax.broadcasted_iota(jnp.int32, shape, 0)
    lane = lanes_of(shape)
    digits = jnp.where(lane == 0, high, jnp.where(lane == 1, low, 0.0))
    tail = jnp.where(row == 0, normed(clean), jnp.where(row == 1, digits, 0.0))
    act_ref[KEYS:, :] = tail.astype(BF16)
    key = lax.broadcasted_iota(jnp.int32, (LANES, LANES), 0)
    hot = (key == flat_ref[...]).astype(F32)
    count_ref[...] = lax.dot_general(
        jnp.ones((8, LANES), F32), hot, (((1,), (1,)), ((), ())), preferred_element_type=F32
    )


def normed_rows(answer_ids, clean_resid, delta_table, norm_gain, flat):
    features = clean_resid.shape[1]
    return pl.pallas_call(
        norm_kernel,
        out_shape=(
            jax.ShapeDtypeStruct((ROWS, features), BF16),
            jax.ShapeDtypeStruct((8, LANES), F32),
        ),
        in_specs=[SMEM, VMEM, VMEM, VMEM, VMEM],
        out_specs=(VMEM, VMEM),
        name="norm",
    )(answer_ids, clean_resid, delta_table, norm_gain, flat)


def score_kernel(*refs):
    acts, (w_ref, out_ref, a_buf, w_buf, l_buf) = refs[:SUBS], refs[SUBS:]
    depth = (w_ref.shape[1] - 8) // FULL
    groups = depth // 8
    copies = out_ref.shape[0]
    me = lax.axis_index("cells")
    sub = me % SUBS
    start = lax.axis_index("vocab") * (SUBS * (FULL * LANES + LEFT))
    for j in range(SUBS):
        a_buf[j * ROWS : (j + 1) * ROWS, :] = acts[j][...]
    for i in range(PLANE):
        rows = slice(i * depth, (i + 1) * depth)
        for k in range(FULL):
            w_buf[rows, k * LANES : (k + 1) * LANES] = w_ref[i, k * depth : (k + 1) * depth, :]
        left = w_ref[i, FULL * depth :, :].astype(F32)
        pieces = [left] + [pltpu.roll(left, LANES - LEFT * a, 1) for a in range(1, groups)]
        w_buf[rows, FULL * LANES :] = jnp.concatenate(pieces, axis=0).astype(BF16)
    l_buf[...] = jnp.dot(a_buf[...], w_buf[...], preferred_element_type=F32)

    width = (FULL + 1) * LANES
    lane = lanes_of((1, width))
    kept = lane < FULL * LANES + LEFT
    column = jnp.where(
        lane < FULL * LANES,
        start + sub * (FULL * LANES) + lane,
        start + SUBS * FULL * LANES + sub * LEFT + lane - FULL * LANES,
    ).astype(F32)
    eye = lax.broadcasted_iota(jnp.int32, (LANES, LANES), 0) == lanes_of((LANES, LANES))
    for t in range(YS):
        parts = []
        for d in range(CORES):
            at = (t * CORES + d) * ROWS
            clean = jnp.where(kept, l_buf[at + KEYS : at + KEYS + 1, :], NEG)
            max_clean = jnp.max(clean, axis=-1, keepdims=True)
            weight = jnp.exp(clean - max_clean)
            sum_clean = jnp.sum(weight, axis=-1, keepdims=True)
            weight = weight * (1.0 / sum_clean)
            clean_lse = max_clean + jnp.log(sum_clean)
            digits = acts[t * CORES + d][KEYS + 1 : KEYS + 2, 0:LANES].astype(F32)
            answer = digits[:, 0:1] * 256.0 + digits[:, 1:2]
            logits = jnp.where(kept, l_buf[at : at + KEYS, :], NEG)
            max_patch = jnp.max(logits, axis=-1, keepdims=True)
            sum_patch = jnp.sum(jnp.exp(logits - max_patch), axis=-1, keepdims=True)
            cross = jnp.sum(weight * (clean - logits), axis=-1, keepdims=True)
            picked = jnp.where((column == answer) & kept, logits, 0.0)
            parts.append(
                (
                    max_patch + jnp.log(sum_patch),
                    cross,
                    jnp.sum(picked, axis=-1, keepdims=True),
                    jnp.broadcast_to(clean_lse, (KEYS, 1)),
                )
            )
        for k in range(4):
            both = jnp.concatenate([parts[0][k], parts[1][k]], axis=0)
            line = jnp.sum(jnp.where(eye, both, 0.0), axis=0, keepdims=True)
            for i in range(copies):
                out_ref[i, 4 * k + t : 4 * k + t + 1, :] = line


def scored(acts, weights, copies):
    depth = (weights.shape[1] - 8) // FULL
    features = acts[0].shape[1]
    return pl.pallas_call(
        score_kernel,
        out_shape=jax.ShapeDtypeStruct((copies, 16, LANES), F32),
        in_specs=[VMEM] * (SUBS + 1),
        out_specs=VMEM,
        scratch_shapes=[
            pltpu.VMEM((SUBS * ROWS, features), BF16),
            pltpu.VMEM((PLANE * depth, (FULL + 1) * LANES), BF16),
            pltpu.VMEM((SUBS * ROWS, (FULL + 1) * LANES), F32),
        ],
        name="score",
    )(*acts, weights)


def merged(lse, cross, answer, clean_lse):
    top = jnp.max(lse, axis=0)
    lse = top + jnp.log(jnp.sum(jnp.exp(lse - top), axis=0))
    top = jnp.max(clean_lse, axis=0)
    weight = jnp.exp(clean_lse - top)
    total = jnp.sum(weight, axis=0)
    cross = jnp.sum(weight * cross, axis=0) / total
    return lse, cross, jnp.sum(answer, axis=0), top + jnp.log(total)


def merge_kernel(in_ref, count_ref, out_ref):
    me = lax.axis_index("cells")
    y, core = (me // CORES) % YS, me % CORES
    stats = merged(*(in_ref[:, 4 * k : 4 * k + 4, :] for k in range(4)))
    lines = []
    for value in stats:
        value = jnp.where(core == 1, pltpu.roll(value, KEYS, 1), value)
        placed = value
        for shift in range(1, YS):
            turned = jnp.concatenate([value[YS - shift :], value[: YS - shift]], axis=0)
            placed = jnp.where(y == shift, turned, placed)
        lines.append(placed)
    lane = lanes_of((8, LANES))
    count = count_ref[...]
    count = jnp.where(core == 1, pltpu.roll(count, KEYS, 1), count)
    count = jnp.where(lane // KEYS == core, count, 0.0)
    for i in range(out_ref.shape[0]):
        for k in range(4):
            out_ref[i, 4 * k : 4 * k + 4, :] = lines[k]
        out_ref[i, 16:, :] = count


def merged_over_vocab(pieces, count):
    return pl.pallas_call(
        merge_kernel,
        out_shape=jax.ShapeDtypeStruct((PLANE, 24, LANES), F32),
        in_specs=[VMEM, VMEM],
        out_specs=VMEM,
        name="merge",
    )(pieces, count)


def finish_kernel(in_ref, flat_ref, out_ref, total_ref):
    me = lax.axis_index("cells")
    row = lax.broadcasted_iota(jnp.int32, (YS, LANES), 0)
    own_row = (me // CORES) % YS
    total = jnp.zeros((YS, LANES), F32)
    own_div = jnp.zeros((YS, LANES), F32)
    own_log = jnp.zeros((YS, LANES), F32)
    for x in range(XS):
        group = slice(x * SUBS, (x + 1) * SUBS)
        lse, cross, answer, clean_lse = merged(
            *(in_ref[group, 4 * k : 4 * k + 4, :] for k in range(4))
        )
        divergence = cross - clean_lse + lse
        count = jnp.concatenate(
            [
                in_ref[x * SUBS + CORES * y, 16:17, :] + in_ref[x * SUBS + CORES * y + 1, 16:17, :]
                for y in range(YS)
            ],
            axis=0,
        )
        total = total + count * divergence
        mine = (row == own_row) & (me // SUBS == x)
        own_div = jnp.where(mine, divergence, own_div)
        own_log = jnp.where(mine, answer - lse, own_log)
    total = jnp.sum(jnp.sum(total, axis=0, keepdims=True), axis=1, keepdims=True)
    total_ref[...] = jnp.broadcast_to(total, total_ref.shape)
    own = jnp.concatenate(
        [
            jnp.sum(own_div, axis=0, keepdims=True),
            jnp.sum(own_log, axis=0, keepdims=True),
            jnp.zeros((6, LANES), F32),
        ],
        axis=0,
    )
    own = jnp.where(me % CORES == 1, pltpu.roll(own, KEYS, 1), own)
    key = lax.broadcasted_iota(jnp.int32, (LANES, LANES), 0)
    hot = (key == flat_ref[...]).astype(F32)
    out_ref[...] = jnp.dot(own, hot, preferred_element_type=F32, precision=lax.Precision.HIGHEST)


def finished(pieces, flat):
    return pl.pallas_call(
        finish_kernel,
        out_shape=(
            jax.ShapeDtypeStruct((8, LANES), F32),
            jax.ShapeDtypeStruct((8, LANES), F32),
        ),
        in_specs=[VMEM, VMEM],
        out_specs=(VMEM, VMEM),
        name="finish",
    )(pieces, flat)


def moved(value, to):
    return lax.ppermute(value, "cells", [(i, to(i)) for i in range(PLANE)])


def along_y(step):
    def to(i):
        x, y, core = i // SUBS, (i // CORES) % YS, i % CORES
        return x * SUBS + ((y - step) % YS) * CORES + core

    return to


def on_device(clean_resid, path_delta, layer_index, pos_index, answer_ids, norm_gain, unembed):
    position_count = path_delta.shape[2]
    features = clean_resid.shape[1]
    cell_count = layer_index.shape[0]
    vocab_size = lax.axis_size("vocab")
    weights = lax.all_to_all(packed(unembed), "cells", 0, 0, tiled=True)
    flat = jnp.pad(
        layer_index * position_count + pos_index,
        (0, LANES - cell_count),
        constant_values=-1,
    ).reshape(1, LANES)
    act, count = normed_rows(
        answer_ids,
        clean_resid,
        path_delta.reshape(KEYS, features),
        norm_gain.reshape(1, features),
        flat,
    )
    same = [act] + [moved(act, along_y(step)) for step in range(1, YS)]
    other = [moved(value, lambda i: i ^ 1) for value in same]
    acts = [value for pair in zip(same, other) for value in pair]
    stats = scored(acts, weights, vocab_size)
    stats = lax.all_to_all(stats, "vocab", 0, 0, tiled=True)
    pieces = merged_over_vocab(stats, count)
    pieces = lax.all_to_all(pieces, "cells", 0, 0, tiled=True)
    out, total = finished(pieces, flat)
    return out[0, :cell_count], out[1, :cell_count], total[0, 0]


def solution(mesh):
    in_specs = (
        P("cells", None),
        P("cells", None, None, None),
        P("cells"),
        P("cells"),
        P("cells"),
        P(),
        P("cells", "vocab"),
    )
    out_specs = (P("cells"), P("cells"), P())
    return jax.shard_map(
        on_device, mesh=mesh, in_specs=in_specs, out_specs=out_specs, check_vma=False
    )
```

```python
import functools

import jax
import jax.numpy as jnp
from jax import lax
from jax.experimental import pallas as pl
from jax.experimental.pallas import tpu as pltpu
from jax.sharding import PartitionSpec as P


XS, YS, CORES = 4, 4, 2
SUBS = YS * CORES
PLANE = XS * SUBS
LANES = 128
KEYS = 64
ROWS = 72
FULL = 3
LEFT = LANES // SUBS
NEG = -1e30
F32 = jnp.float32
BF16 = jnp.bfloat16
MIB = 1 << 20
VMEM = pl.BlockSpec(memory_space=pltpu.VMEM)
SMEM = pl.BlockSpec(memory_space=pltpu.SMEM)


def lanes_of(shape):
    return lax.broadcasted_iota(jnp.int32, shape, len(shape) - 1)


def pack_kernel(u_ref, out_ref):
    depth = u_ref.shape[0]
    groups = depth // 8
    last = u_ref[:, SUBS * FULL * LANES :].astype(F32)
    lane = lanes_of((8, LANES))
    for sub in range(SUBS):
        left = jnp.zeros((8, LANES), F32)
        for a in range(groups):
            piece = pltpu.roll(last[8 * a : 8 * a + 8], (LEFT * (a - sub)) % LANES, 1)
            left = jnp.where(lane // LEFT == a, piece, left)
        left = left.astype(BF16)
        for x in range(XS):
            to = x * SUBS + sub
            for k in range(FULL):
                at = (sub * FULL + k) * LANES
                out_ref[to, k * depth : (k + 1) * depth, :] = u_ref[:, at : at + LANES]
            out_ref[to, FULL * depth :, :] = left


def packed(unembed):
    depth = unembed.shape[0]
    return pl.pallas_call(
        pack_kernel,
        out_shape=jax.ShapeDtypeStruct((PLANE, FULL * depth + 8, LANES), BF16),
        in_specs=[VMEM],
        out_specs=VMEM,
        compiler_params=pltpu.CompilerParams(vmem_limit_bytes=8 * MIB),
        name="pack",
    )(unembed)


def key_hits(layer_ref, pos_ref, position_count):
    flat = layer_ref[...] * position_count + pos_ref[...]
    key = lax.broadcasted_iota(jnp.int32, (LANES, flat.shape[1]), 0)
    return (key == flat).astype(F32)


def as_line(column):
    square = (LANES, LANES)
    eye = lax.broadcasted_iota(jnp.int32, square, 0) == lanes_of(square)
    return jnp.sum(jnp.where(eye, column, 0.0), axis=0, keepdims=True)


def norm_kernel(answer_ref, clean_ref, delta_ref, gain_ref, act_ref):
    features = clean_ref.shape[1]
    clean = clean_ref[...]
    gain = gain_ref[...]

    def normed(values):
        mean_square = jnp.sum(values * values, axis=-1, keepdims=True) * (1.0 / features)
        return values * lax.rsqrt(mean_square + 1e-06) * gain

    patched = normed(clean + delta_ref[...].astype(F32)).astype(BF16)
    answer = answer_ref[0]
    high = lax.shift_right_logical(answer, 8).astype(F32)
    low = (answer & 255).astype(F32)
    shape = (ROWS - KEYS, features)
    row = lax.broadcasted_iota(jnp.int32, shape, 0)
    lane = lanes_of(shape)
    digits = jnp.where(lane == 0, high, jnp.where(lane == 1, low, 0.0))
    tail = jnp.where(row == 0, normed(clean), jnp.where(row == 1, digits, 0.0)).astype(BF16)
    act_ref[:KEYS, :] = patched
    act_ref[KEYS:, :] = tail


def normed_rows(answer_ids, clean_resid, delta_table, norm_gain):
    features = clean_resid.shape[1]
    return pl.pallas_call(
        norm_kernel,
        out_shape=jax.ShapeDtypeStruct((ROWS, features), BF16),
        in_specs=[SMEM, VMEM, VMEM, VMEM],
        out_specs=VMEM,
        compiler_params=pltpu.CompilerParams(vmem_limit_bytes=8 * MIB),
        name="norm",
    )(answer_ids, clean_resid, delta_table, norm_gain)


def score_kernel(*refs):
    acts, (w_ref, out_ref, a_buf, w_buf, l_buf) = refs[:SUBS], refs[SUBS:]
    depth = (w_ref.shape[1] - 8) // FULL
    groups = depth // 8
    copies = out_ref.shape[0]
    me = lax.axis_index("cells")
    sub = me % SUBS
    start = lax.axis_index("vocab") * (SUBS * (FULL * LANES + LEFT))
    for i in range(PLANE):
        rows = slice(i * depth, (i + 1) * depth)
        for k in range(FULL):
            w_buf[rows, k * LANES : (k + 1) * LANES] = w_ref[i, k * depth : (k + 1) * depth, :]
        left = w_ref[i, FULL * depth :, :].astype(F32)
        pieces = [left] + [pltpu.roll(left, LANES - LEFT * a, 1) for a in range(1, groups)]
        w_buf[rows, FULL * LANES :] = jnp.concatenate(pieces, axis=0).astype(BF16)
    for j in range(SUBS):
        a_buf[j * ROWS : (j + 1) * ROWS, :] = acts[j][...]
    l_buf[...] = jnp.dot(a_buf[...], w_buf[...], preferred_element_type=F32)

    width = (FULL + 1) * LANES
    lane = lanes_of((1, width))
    kept = lane < FULL * LANES + LEFT
    column = jnp.where(
        lane < FULL * LANES,
        start + sub * (FULL * LANES) + lane,
        start + SUBS * FULL * LANES + sub * LEFT + lane - FULL * LANES,
    ).astype(F32)
    for t in range(YS):
        parts = []
        for d in range(CORES):
            at = (d * YS + t) * ROWS
            clean = jnp.where(kept, l_buf[at + KEYS : at + KEYS + 1, :], NEG)
            max_clean = jnp.max(clean, axis=-1, keepdims=True)
            weight = jnp.exp(clean - max_clean)
            sum_clean = jnp.sum(weight, axis=-1, keepdims=True)
            weight = weight * (1.0 / sum_clean)
            clean_lse = max_clean + jnp.log(sum_clean)
            tail = acts[d * YS + t][KEYS:, 0:LANES].astype(F32)
            digits = tail[1:2]
            answer = digits[:, 0:1] * 256.0 + digits[:, 1:2]
            logits = jnp.where(kept, l_buf[at : at + KEYS, :], NEG)
            max_patch = jnp.max(logits, axis=-1, keepdims=True)
            sum_patch = jnp.sum(jnp.exp(logits - max_patch), axis=-1, keepdims=True)
            cross = jnp.sum(weight * (clean - logits), axis=-1, keepdims=True)
            picked = jnp.where((column == answer) & kept, logits, 0.0)
            parts.append(
                (
                    max_patch + jnp.log(sum_patch),
                    cross,
                    jnp.sum(picked, axis=-1, keepdims=True),
                    jnp.broadcast_to(clean_lse, (KEYS, 1)),
                )
            )
        for k in range(4):
            both = jnp.concatenate([parts[0][k], parts[1][k]], axis=0)
            line = as_line(both)
            for i in range(copies):
                out_ref[i, 4 * k + t : 4 * k + t + 1, :] = line


def scored(acts, weights, copies):
    depth = (weights.shape[1] - 8) // FULL
    return pl.pallas_call(
        score_kernel,
        out_shape=jax.ShapeDtypeStruct((copies, 16, LANES), F32),
        in_specs=[VMEM] * (SUBS + 1),
        out_specs=VMEM,
        scratch_shapes=[
            pltpu.VMEM((SUBS * ROWS, acts[0].shape[1]), BF16),
            pltpu.VMEM((PLANE * depth, (FULL + 1) * LANES), BF16),
            pltpu.VMEM((2 * YS * ROWS, (FULL + 1) * LANES), F32),
        ],
        compiler_params=pltpu.CompilerParams(vmem_limit_bytes=24 * MIB),
        name="score",
    )(*acts, weights)


def merged(lse, cross, answer, clean_lse):
    top = jnp.max(lse, axis=0)
    lse = top + jnp.log(jnp.sum(jnp.exp(lse - top), axis=0))
    top = jnp.max(clean_lse, axis=0)
    weight = jnp.exp(clean_lse - top)
    total = jnp.sum(weight, axis=0)
    cross = jnp.sum(weight * cross, axis=0) / total
    return lse, cross, jnp.sum(answer, axis=0), top + jnp.log(total)


def merge_kernel(in_ref, layer_ref, pos_ref, out_ref, *, position_count):
    me = lax.axis_index("cells")
    y, core = (me // CORES) % YS, me % CORES
    lines = []
    for value in merged(*(in_ref[:, 4 * k : 4 * k + 4, :] for k in range(4))):
        value = jnp.where(core == 1, pltpu.roll(value, KEYS, 1), value)
        placed = value
        for shift in range(1, YS):
            turned = jnp.concatenate([value[YS - shift :], value[: YS - shift]], axis=0)
            placed = jnp.where(y == shift, turned, placed)
        lines.append(placed)
    hits = key_hits(layer_ref, pos_ref, position_count)
    count = as_line(jnp.sum(hits, axis=1, keepdims=True))
    lane = lanes_of((YS, LANES))
    row = lax.broadcasted_iota(jnp.int32, (YS, LANES), 0)
    half = KEYS // 2
    count = jnp.where(row == 0, pltpu.roll(count, half, 1), count)
    lines[3] = jnp.where((lane // half == 1) & (row < 2), count, lines[3])
    for i in range(out_ref.shape[0]):
        for k in range(4):
            out_ref[i, 4 * k : 4 * k + 4, :] = lines[k]


def merged_over_vocab(pieces, layer, pos, position_count):
    return pl.pallas_call(
        functools.partial(merge_kernel, position_count=position_count),
        out_shape=jax.ShapeDtypeStruct((PLANE, 16, LANES), F32),
        in_specs=[VMEM, VMEM, VMEM],
        out_specs=VMEM,
        compiler_params=pltpu.CompilerParams(vmem_limit_bytes=8 * MIB),
        name="merge",
    )(pieces, layer, pos)


def finish_kernel(in_ref, layer_ref, pos_ref, div_ref, log_ref, total_ref, *, position_count):
    me = lax.axis_index("cells")
    shape = (YS, LANES)
    row = lax.broadcasted_iota(jnp.int32, shape, 0)
    lane = lanes_of(shape)
    half = KEYS // 2
    own_row = (me // CORES) % YS
    total = jnp.zeros(shape, F32)
    own_div = jnp.zeros(shape, F32)
    own_log = jnp.zeros(shape, F32)
    for x in range(XS):
        group = slice(x * SUBS, (x + 1) * SUBS)
        clean = in_ref[group, 12:16, :]
        spread = [
            jnp.where(lane % KEYS < half, clean[s], pltpu.roll(clean[s], half, 1))[None]
            for s in range(SUBS)
        ]
        lse, cross, answer, clean_lse = merged(
            *(in_ref[group, 4 * k : 4 * k + 4, :] for k in range(3)),
            jnp.concatenate(spread, axis=0),
        )
        divergence = cross - clean_lse + lse
        for s in range(SUBS):
            y, core = s // CORES, s % CORES
            left = pltpu.roll(clean[s], (core * KEYS - half) % LANES, 1)[0:1]
            right = clean[s][1:2]
            if core == 1:
                right = pltpu.roll(clean[s], KEYS, 1)[1:2]
            count = jnp.where(lane[0:1] % KEYS < half, left, right)
            count = jnp.where(lane[0:1] // KEYS == core, count, 0.0)
            total = total + jnp.where(row == y, count * divergence, 0.0)
        mine = (row == own_row) & (me // SUBS == x)
        own_div = jnp.where(mine, divergence, own_div)
        own_log = jnp.where(mine, answer - lse, own_log)
    total_ref[...] = jnp.sum(jnp.sum(total, axis=0, keepdims=True), axis=1, keepdims=True)
    own = jnp.concatenate(
        [
            jnp.sum(own_div, axis=0, keepdims=True),
            jnp.sum(own_log, axis=0, keepdims=True),
            jnp.zeros((6, LANES), F32),
        ],
        axis=0,
    )
    own = jnp.where(me % CORES == 1, pltpu.roll(own, KEYS, 1), own)
    hits = key_hits(layer_ref, pos_ref, position_count)
    out = jnp.dot(own, hits, preferred_element_type=F32, precision=lax.Precision.HIGHEST)
    div_ref[...] = out[0]
    log_ref[...] = out[1]


def finished(pieces, layer, pos, position_count):
    cells = layer.shape[1]
    return pl.pallas_call(
        functools.partial(finish_kernel, position_count=position_count),
        out_shape=(
            jax.ShapeDtypeStruct((cells,), F32),
            jax.ShapeDtypeStruct((cells,), F32),
            jax.ShapeDtypeStruct((1, 1), F32),
        ),
        in_specs=[VMEM, VMEM, VMEM],
        out_specs=(VMEM, VMEM, VMEM),
        compiler_params=pltpu.CompilerParams(vmem_limit_bytes=8 * MIB),
        name="finish",
    )(pieces, layer, pos)


def moved(value, to):
    return lax.ppermute(value, "cells", [(i, to(i)) for i in range(PLANE)])


def along_y(step):
    def to(i):
        x, y, core = i // SUBS, (i // CORES) % YS, i % CORES
        return x * SUBS + ((y - step) % YS) * CORES + core

    return to


def on_device(clean_resid, path_delta, layer_index, pos_index, answer_ids, norm_gain, unembed):
    position_count = path_delta.shape[2]
    features = clean_resid.shape[1]
    act = normed_rows(
        answer_ids,
        clean_resid,
        path_delta.reshape(KEYS, features),
        norm_gain.reshape(1, features),
    )
    same = [act]
    for step in range(1, YS):
        same.append(moved(act, along_y(step)))
    weights = lax.all_to_all(packed(unembed), "cells", 0, 0, tiled=True)
    other = []
    for step in range(YS):
        other.append(moved(same[step], lambda i: i ^ 1))
    stats = scored(same + other, weights, lax.axis_size("vocab"))
    stats = lax.all_to_all(stats, "vocab", 0, 0, tiled=True)
    layer, pos = layer_index.reshape(1, -1), pos_index.reshape(1, -1)
    pieces = merged_over_vocab(stats, layer, pos, position_count)
    pieces = lax.all_to_all(pieces, "cells", 0, 0, tiled=True)
    divergence, answer_logprob, total = finished(pieces, layer, pos, position_count)
    return divergence, answer_logprob, total.reshape(())


def solution(mesh):
    in_specs = (
        P("cells", None),
        P("cells", None, None, None),
        P("cells"),
        P("cells"),
        P("cells"),
        P(),
        P("cells", "vocab"),
    )
    out_specs = (P("cells"), P("cells"), P())
    return jax.shard_map(
        on_device, mesh=mesh, in_specs=in_specs, out_specs=out_specs, check_vma=False
    )
```

```python
import functools

import jax
import jax.numpy as jnp
from jax import lax
from jax.experimental import pallas as pl
from jax.experimental.pallas import tpu as pltpu
from jax.sharding import PartitionSpec as P


XS, YS, CORES = 4, 4, 2
SUBS = YS * CORES
PLANE = XS * SUBS
LANES = 128
KEYS = 64
ROWS = 72
FULL = 3
LEFT = LANES // SUBS
NEG = -1e30
F32 = jnp.float32
BF16 = jnp.bfloat16
MIB = 1 << 20
VMEM = pl.BlockSpec(memory_space=pltpu.VMEM)
SMEM = pl.BlockSpec(memory_space=pltpu.SMEM)


def lanes_of(shape):
    return lax.broadcasted_iota(jnp.int32, shape, len(shape) - 1)


def pack_kernel(u_ref, out_ref):
    depth = u_ref.shape[0]
    groups = depth // 8
    last = u_ref[:, SUBS * FULL * LANES :].astype(F32)
    lane = lanes_of((8, LANES))
    for sub in range(SUBS):
        left = jnp.zeros((8, LANES), F32)
        for a in range(groups):
            piece = pltpu.roll(last[8 * a : 8 * a + 8], (LEFT * (a - sub)) % LANES, 1)
            left = jnp.where(lane // LEFT == a, piece, left)
        left = left.astype(BF16)
        for x in range(XS):
            to = x * SUBS + sub
            for k in range(FULL):
                at = (sub * FULL + k) * LANES
                out_ref[to, k * depth : (k + 1) * depth, :] = u_ref[:, at : at + LANES]
            out_ref[to, FULL * depth :, :] = left


def packed(unembed):
    depth = unembed.shape[0]
    return pl.pallas_call(
        pack_kernel,
        out_shape=jax.ShapeDtypeStruct((PLANE, FULL * depth + 8, LANES), BF16),
        in_specs=[VMEM],
        out_specs=VMEM,
        compiler_params=pltpu.CompilerParams(vmem_limit_bytes=8 * MIB),
        name="pack",
    )(unembed)


def key_hits(layer_ref, pos_ref, position_count):
    flat = layer_ref[...] * position_count + pos_ref[...]
    key = lax.broadcasted_iota(jnp.int32, (LANES, flat.shape[1]), 0)
    return (key == flat).astype(F32)


def as_line(column):
    square = (LANES, LANES)
    eye = lax.broadcasted_iota(jnp.int32, square, 0) == lanes_of(square)
    return jnp.sum(jnp.where(eye, column, 0.0), axis=0, keepdims=True)


def norm_kernel(answer_ref, clean_ref, delta_ref, gain_ref, act_ref):
    features = clean_ref.shape[1]
    clean = clean_ref[...]
    gain = gain_ref[...]

    def normed(values):
        mean_square = jnp.sum(values * values, axis=-1, keepdims=True) * (1.0 / features)
        return values * lax.rsqrt(mean_square + 1e-06) * gain

    patched = normed(clean + delta_ref[...].astype(F32)).astype(BF16)
    answer = answer_ref[0]
    high = lax.shift_right_logical(answer, 8).astype(F32)
    low = (answer & 255).astype(F32)
    shape = (ROWS - KEYS, features)
    row = lax.broadcasted_iota(jnp.int32, shape, 0)
    lane = lanes_of(shape)
    digits = jnp.where(lane == 0, high, jnp.where(lane == 1, low, 0.0))
    tail = jnp.where(row == 0, normed(clean), jnp.where(row == 1, digits, 0.0)).astype(BF16)
    act_ref[:KEYS, :] = patched
    act_ref[KEYS:, :] = tail


def normed_rows(answer_ids, clean_resid, delta_table, norm_gain):
    features = clean_resid.shape[1]
    return pl.pallas_call(
        norm_kernel,
        out_shape=jax.ShapeDtypeStruct((ROWS, features), BF16),
        in_specs=[SMEM, VMEM, VMEM, VMEM],
        out_specs=VMEM,
        compiler_params=pltpu.CompilerParams(vmem_limit_bytes=8 * MIB),
        name="norm",
    )(answer_ids, clean_resid, delta_table, norm_gain)


def stack_kernel(*refs):
    acts, out_ref = refs[:SUBS], refs[SUBS]
    for j in range(SUBS):
        out_ref[j * ROWS : (j + 1) * ROWS, :] = acts[j][...]


def stacked(acts):
    return pl.pallas_call(
        stack_kernel,
        out_shape=jax.ShapeDtypeStruct((SUBS * ROWS, acts[0].shape[1]), BF16),
        in_specs=[VMEM] * SUBS,
        out_specs=VMEM,
        compiler_params=pltpu.CompilerParams(vmem_limit_bytes=8 * MIB),
        name="stack",
    )(*acts)


def score_kernel(a_ref, w_ref, out_ref, w_buf, l_buf):
    depth = (w_ref.shape[1] - 8) // FULL
    groups = depth // 8
    copies = out_ref.shape[0]
    me = lax.axis_index("cells")
    sub = me % SUBS
    start = lax.axis_index("vocab") * (SUBS * (FULL * LANES + LEFT))
    for i in range(PLANE):
        rows = slice(i * depth, (i + 1) * depth)
        for k in range(FULL):
            w_buf[rows, k * LANES : (k + 1) * LANES] = w_ref[i, k * depth : (k + 1) * depth, :]
        left = w_ref[i, FULL * depth :, :].astype(F32)
        pieces = [left] + [pltpu.roll(left, LANES - LEFT * a, 1) for a in range(1, groups)]
        w_buf[rows, FULL * LANES :] = jnp.concatenate(pieces, axis=0).astype(BF16)
    l_buf[...] = jnp.dot(a_ref[...], w_buf[...], preferred_element_type=F32)

    width = (FULL + 1) * LANES
    lane = lanes_of((1, width))
    kept = lane < FULL * LANES + LEFT
    column = jnp.where(
        lane < FULL * LANES,
        start + sub * (FULL * LANES) + lane,
        start + SUBS * FULL * LANES + sub * LEFT + lane - FULL * LANES,
    ).astype(F32)
    for t in range(YS):
        parts = []
        for d in range(CORES):
            at = (d * YS + t) * ROWS
            clean = jnp.where(kept, l_buf[at + KEYS : at + KEYS + 1, :], NEG)
            max_clean = jnp.max(clean, axis=-1, keepdims=True)
            weight = jnp.exp(clean - max_clean)
            sum_clean = jnp.sum(weight, axis=-1, keepdims=True)
            weight = weight * (1.0 / sum_clean)
            clean_lse = max_clean + jnp.log(sum_clean)
            tail = a_ref[at + KEYS : at + ROWS, 0:LANES].astype(F32)
            digits = tail[1:2]
            answer = digits[:, 0:1] * 256.0 + digits[:, 1:2]
            logits = jnp.where(kept, l_buf[at : at + KEYS, :], NEG)
            max_patch = jnp.max(logits, axis=-1, keepdims=True)
            sum_patch = jnp.sum(jnp.exp(logits - max_patch), axis=-1, keepdims=True)
            cross = jnp.sum(weight * (clean - logits), axis=-1, keepdims=True)
            picked = jnp.where((column == answer) & kept, logits, 0.0)
            parts.append(
                (
                    max_patch + jnp.log(sum_patch),
                    cross,
                    jnp.sum(picked, axis=-1, keepdims=True),
                    jnp.broadcast_to(clean_lse, (KEYS, 1)),
                )
            )
        for k in range(4):
            both = jnp.concatenate([parts[0][k], parts[1][k]], axis=0)
            line = as_line(both)
            for i in range(copies):
                out_ref[i, 4 * k + t : 4 * k + t + 1, :] = line


def scored(rows, weights, copies):
    depth = (weights.shape[1] - 8) // FULL
    return pl.pallas_call(
        score_kernel,
        out_shape=jax.ShapeDtypeStruct((copies, 16, LANES), F32),
        in_specs=[VMEM, VMEM],
        out_specs=VMEM,
        scratch_shapes=[
            pltpu.VMEM((PLANE * depth, (FULL + 1) * LANES), BF16),
            pltpu.VMEM((2 * YS * ROWS, (FULL + 1) * LANES), F32),
        ],
        compiler_params=pltpu.CompilerParams(vmem_limit_bytes=12 * MIB),
        name="score",
    )(rows, weights)


def merged(lse, cross, answer, clean_lse):
    top = jnp.max(lse, axis=0)
    lse = top + jnp.log(jnp.sum(jnp.exp(lse - top), axis=0))
    top = jnp.max(clean_lse, axis=0)
    weight = jnp.exp(clean_lse - top)
    total = jnp.sum(weight, axis=0)
    cross = jnp.sum(weight * cross, axis=0) / total
    return lse, cross, jnp.sum(answer, axis=0), top + jnp.log(total)


def merge_kernel(in_ref, layer_ref, pos_ref, out_ref, *, position_count):
    me = lax.axis_index("cells")
    y, core = (me // CORES) % YS, me % CORES
    lines = []
    for value in merged(*(in_ref[:, 4 * k : 4 * k + 4, :] for k in range(4))):
        value = jnp.where(core == 1, pltpu.roll(value, KEYS, 1), value)
        placed = value
        for shift in range(1, YS):
            turned = jnp.concatenate([value[YS - shift :], value[: YS - shift]], axis=0)
            placed = jnp.where(y == shift, turned, placed)
        lines.append(placed)
    hits = key_hits(layer_ref, pos_ref, position_count)
    count = as_line(jnp.sum(hits, axis=1, keepdims=True))
    lane = lanes_of((YS, LANES))
    row = lax.broadcasted_iota(jnp.int32, (YS, LANES), 0)
    half = KEYS // 2
    count = jnp.where(row == 0, pltpu.roll(count, half, 1), count)
    lines[3] = jnp.where((lane // half == 1) & (row < 2), count, lines[3])
    for i in range(out_ref.shape[0]):
        for k in range(4):
            out_ref[i, 4 * k : 4 * k + 4, :] = lines[k]


def merged_over_vocab(pieces, layer, pos, position_count):
    return pl.pallas_call(
        functools.partial(merge_kernel, position_count=position_count),
        out_shape=jax.ShapeDtypeStruct((PLANE, 16, LANES), F32),
        in_specs=[VMEM, VMEM, VMEM],
        out_specs=VMEM,
        compiler_params=pltpu.CompilerParams(vmem_limit_bytes=8 * MIB),
        name="merge",
    )(pieces, layer, pos)


def finish_kernel(in_ref, layer_ref, pos_ref, div_ref, log_ref, total_ref, *, position_count):
    me = lax.axis_index("cells")
    shape = (YS, LANES)
    row = lax.broadcasted_iota(jnp.int32, shape, 0)
    lane = lanes_of(shape)
    half = KEYS // 2
    own_row = (me // CORES) % YS
    total = jnp.zeros(shape, F32)
    own_div = jnp.zeros(shape, F32)
    own_log = jnp.zeros(shape, F32)
    for x in range(XS):
        group = slice(x * SUBS, (x + 1) * SUBS)
        clean = in_ref[group, 12:16, :]
        spread = [
            jnp.where(lane % KEYS < half, clean[s], pltpu.roll(clean[s], half, 1))[None]
            for s in range(SUBS)
        ]
        lse, cross, answer, clean_lse = merged(
            *(in_ref[group, 4 * k : 4 * k + 4, :] for k in range(3)),
            jnp.concatenate(spread, axis=0),
        )
        divergence = cross - clean_lse + lse
        for s in range(SUBS):
            y, core = s // CORES, s % CORES
            left = pltpu.roll(clean[s], (core * KEYS - half) % LANES, 1)[0:1]
            right = clean[s][1:2]
            if core == 1:
                right = pltpu.roll(clean[s], KEYS, 1)[1:2]
            count = jnp.where(lane[0:1] % KEYS < half, left, right)
            count = jnp.where(lane[0:1] // KEYS == core, count, 0.0)
            total = total + jnp.where(row == y, count * divergence, 0.0)
        mine = (row == own_row) & (me // SUBS == x)
        own_div = jnp.where(mine, divergence, own_div)
        own_log = jnp.where(mine, answer - lse, own_log)
    total_ref[...] = jnp.sum(jnp.sum(total, axis=0, keepdims=True), axis=1, keepdims=True)
    own = jnp.concatenate(
        [
            jnp.sum(own_div, axis=0, keepdims=True),
            jnp.sum(own_log, axis=0, keepdims=True),
            jnp.zeros((6, LANES), F32),
        ],
        axis=0,
    )
    own = jnp.where(me % CORES == 1, pltpu.roll(own, KEYS, 1), own)
    hits = key_hits(layer_ref, pos_ref, position_count)
    out = jnp.dot(own, hits, preferred_element_type=F32, precision=lax.Precision.HIGHEST)
    div_ref[...] = out[0]
    log_ref[...] = out[1]


def finished(pieces, layer, pos, position_count):
    cells = layer.shape[1]
    return pl.pallas_call(
        functools.partial(finish_kernel, position_count=position_count),
        out_shape=(
            jax.ShapeDtypeStruct((cells,), F32),
            jax.ShapeDtypeStruct((cells,), F32),
            jax.ShapeDtypeStruct((1, 1), F32),
        ),
        in_specs=[VMEM, VMEM, VMEM],
        out_specs=(VMEM, VMEM, VMEM),
        compiler_params=pltpu.CompilerParams(vmem_limit_bytes=8 * MIB),
        name="finish",
    )(pieces, layer, pos)


def moved(value, to):
    return lax.ppermute(value, "cells", [(i, to(i)) for i in range(PLANE)])


def along_y(step):
    def to(i):
        x, y, core = i // SUBS, (i // CORES) % YS, i % CORES
        return x * SUBS + ((y - step) % YS) * CORES + core

    return to


def on_device(clean_resid, path_delta, layer_index, pos_index, answer_ids, norm_gain, unembed):
    position_count = path_delta.shape[2]
    features = clean_resid.shape[1]
    act = normed_rows(
        answer_ids,
        clean_resid,
        path_delta.reshape(KEYS, features),
        norm_gain.reshape(1, features),
    )
    same = [act]
    for step in range(1, YS):
        same.append(moved(act, along_y(step)))
    weights = lax.all_to_all(packed(unembed), "cells", 0, 0, tiled=True)
    other = []
    for step in range(YS):
        other.append(moved(same[step], lambda i: i ^ 1))
    stats = scored(stacked(same + other), weights, lax.axis_size("vocab"))
    stats = lax.all_to_all(stats, "vocab", 0, 0, tiled=True)
    layer, pos = layer_index.reshape(1, -1), pos_index.reshape(1, -1)
    pieces = merged_over_vocab(stats, layer, pos, position_count)
    pieces = lax.all_to_all(pieces, "cells", 0, 0, tiled=True)
    divergence, answer_logprob, total = finished(pieces, layer, pos, position_count)
    return divergence, answer_logprob, total.reshape(())


def solution(mesh):
    in_specs = (
        P("cells", None),
        P("cells", None, None, None),
        P("cells"),
        P("cells"),
        P("cells"),
        P(),
        P("cells", "vocab"),
    )
    out_specs = (P("cells"), P("cells"), P())
    return jax.shard_map(
        on_device, mesh=mesh, in_specs=in_specs, out_specs=out_specs, check_vma=False
    )
```

```python
import functools

import jax
import jax.numpy as jnp
from jax import lax
from jax.experimental import pallas as pl
from jax.experimental.pallas import tpu as pltpu
from jax.sharding import PartitionSpec as P


XS, YS, CORES = 4, 4, 2
SUBS = YS * CORES
PLANE = XS * SUBS
LANES = 128
KEYS = 64
ROWS = 72
FULL = 3
LEFT = LANES // SUBS
NEG = -1e30
F32 = jnp.float32
BF16 = jnp.bfloat16
MIB = 1 << 20
VMEM = pl.BlockSpec(memory_space=pltpu.VMEM)
SMEM = pl.BlockSpec(memory_space=pltpu.SMEM)


def lanes_of(shape):
    return lax.broadcasted_iota(jnp.int32, shape, len(shape) - 1)


def key_hits(layer_ref, pos_ref, position_count):
    flat = layer_ref[...] * position_count + pos_ref[...]
    key = lax.broadcasted_iota(jnp.int32, (LANES, flat.shape[1]), 0)
    return (key == flat).astype(F32)


def as_line(column):
    square = (LANES, LANES)
    eye = lax.broadcasted_iota(jnp.int32, square, 0) == lanes_of(square)
    return jnp.sum(jnp.where(eye, column, 0.0), axis=0, keepdims=True)


def pack_columns(u_ref, out_ref):
    depth = u_ref.shape[0]
    groups = depth // 8
    last = u_ref[:, SUBS * FULL * LANES :].astype(F32)
    lane = lanes_of((8, LANES))
    for sub in range(SUBS):
        left = jnp.zeros((8, LANES), F32)
        for a in range(groups):
            piece = pltpu.roll(last[8 * a : 8 * a + 8], (LEFT * (a - sub)) % LANES, 1)
            left = jnp.where(lane // LEFT == a, piece, left)
        left = left.astype(BF16)
        for x in range(XS):
            to = x * SUBS + sub
            for k in range(FULL):
                at = (sub * FULL + k) * LANES
                out_ref[to, k * depth : (k + 1) * depth, :] = u_ref[:, at : at + LANES]
            out_ref[to, FULL * depth :, :] = left


def norm_rows(answer_ref, clean_ref, delta_ref, gain_ref, act_ref):
    features = clean_ref.shape[1]
    clean = clean_ref[...]
    gain = gain_ref[...]

    def normed(values):
        mean_square = jnp.sum(values * values, axis=-1, keepdims=True) * (1.0 / features)
        return values * lax.rsqrt(mean_square + 1e-06) * gain

    act_ref[:KEYS, :] = normed(clean + delta_ref[...].astype(F32)).astype(BF16)
    answer = answer_ref[0]
    high = lax.shift_right_logical(answer, 8).astype(F32)
    low = (answer & 255).astype(F32)
    shape = (ROWS - KEYS, features)
    row = lax.broadcasted_iota(jnp.int32, shape, 0)
    lane = lanes_of(shape)
    digits = jnp.where(lane == 0, high, jnp.where(lane == 1, low, 0.0))
    tail = jnp.where(row == 0, normed(clean), jnp.where(row == 1, digits, 0.0))
    act_ref[KEYS:, :] = tail.astype(BF16)


def prepare_kernel(answer_ref, *refs):
    sources, (act_ref, pack_ref), buffers, sems = refs[:4], refs[4:6], refs[6:10], refs[10]
    copies = [
        pltpu.make_async_copy(source, buffer, sems.at[k])
        for k, (source, buffer) in enumerate(zip(sources, buffers))
    ]
    for copy in copies:
        copy.start()
    for copy in copies[:3]:
        copy.wait()
    clean, delta, gain, columns = buffers
    norm_rows(answer_ref, clean, delta, gain, act_ref)
    copies[3].wait()
    pack_columns(columns, pack_ref)


def prepared(answer_ids, clean_resid, delta_table, norm_gain, unembed):
    arrays = (clean_resid, delta_table, norm_gain, unembed)
    depth = unembed.shape[0]
    return pl.pallas_call(
        prepare_kernel,
        out_shape=(
            jax.ShapeDtypeStruct((ROWS, clean_resid.shape[1]), BF16),
            jax.ShapeDtypeStruct((PLANE, FULL * depth + 8, LANES), BF16),
        ),
        in_specs=[SMEM] + [pl.BlockSpec(memory_space=pltpu.HBM)] * 4,
        out_specs=(VMEM, VMEM),
        scratch_shapes=[pltpu.VMEM(array.shape, array.dtype) for array in arrays]
        + [pltpu.SemaphoreType.DMA((4,))],
        compiler_params=pltpu.CompilerParams(vmem_limit_bytes=67043328),
        name="prepare",
    )(answer_ids, *arrays)


def stack_kernel(*refs):
    acts, out_ref = refs[:SUBS], refs[SUBS]
    for j in range(SUBS):
        out_ref[j * ROWS : (j + 1) * ROWS, :] = acts[j][...]


def stacked(acts):
    return pl.pallas_call(
        stack_kernel,
        out_shape=jax.ShapeDtypeStruct((SUBS * ROWS, acts[0].shape[1]), BF16),
        in_specs=[VMEM] * SUBS,
        out_specs=VMEM,
        compiler_params=pltpu.CompilerParams(vmem_limit_bytes=8 * MIB),
        name="stack",
    )(*acts)


def score_kernel(a_ref, w_ref, out_ref, w_buf, l_buf):
    depth = (w_ref.shape[1] - 8) // FULL
    groups = depth // 8
    copies = out_ref.shape[0]
    me = lax.axis_index("cells")
    sub = me % SUBS
    start = lax.axis_index("vocab") * (SUBS * (FULL * LANES + LEFT))
    for i in range(PLANE):
        rows = slice(i * depth, (i + 1) * depth)
        for k in range(FULL):
            w_buf[rows, k * LANES : (k + 1) * LANES] = w_ref[i, k * depth : (k + 1) * depth, :]
        left = w_ref[i, FULL * depth :, :].astype(F32)
        pieces = [left] + [pltpu.roll(left, LANES - LEFT * a, 1) for a in range(1, groups)]
        w_buf[rows, FULL * LANES :] = jnp.concatenate(pieces, axis=0).astype(BF16)
    l_buf[...] = jnp.dot(a_ref[...], w_buf[...], preferred_element_type=F32)

    width = (FULL + 1) * LANES
    lane = lanes_of((1, width))
    kept = lane < FULL * LANES + LEFT
    column = jnp.where(
        lane < FULL * LANES,
        start + sub * (FULL * LANES) + lane,
        start + SUBS * FULL * LANES + sub * LEFT + lane - FULL * LANES,
    ).astype(F32)
    for t in range(YS):
        parts = []
        for d in range(CORES):
            at = (d * YS + t) * ROWS
            clean = jnp.where(kept, l_buf[at + KEYS : at + KEYS + 1, :], NEG)
            max_clean = jnp.max(clean, axis=-1, keepdims=True)
            weight = jnp.exp(clean - max_clean)
            sum_clean = jnp.sum(weight, axis=-1, keepdims=True)
            weight = weight * (1.0 / sum_clean)
            clean_lse = max_clean + jnp.log(sum_clean)
            tail = a_ref[at + KEYS : at + ROWS, 0:LANES].astype(F32)
            digits = tail[1:2]
            answer = digits[:, 0:1] * 256.0 + digits[:, 1:2]
            logits = jnp.where(kept, l_buf[at : at + KEYS, :], NEG)
            max_patch = jnp.max(logits, axis=-1, keepdims=True)
            sum_patch = jnp.sum(jnp.exp(logits - max_patch), axis=-1, keepdims=True)
            cross = jnp.sum(weight * (clean - logits), axis=-1, keepdims=True)
            picked = jnp.where((column == answer) & kept, logits, 0.0)
            parts.append(
                (
                    max_patch + jnp.log(sum_patch),
                    cross,
                    jnp.sum(picked, axis=-1, keepdims=True),
                    jnp.broadcast_to(clean_lse, (KEYS, 1)),
                )
            )
        for k in range(4):
            both = jnp.concatenate([parts[0][k], parts[1][k]], axis=0)
            line = as_line(both)
            for i in range(copies):
                out_ref[i, 4 * k + t : 4 * k + t + 1, :] = line


def scored(rows, weights, copies):
    depth = (weights.shape[1] - 8) // FULL
    return pl.pallas_call(
        score_kernel,
        out_shape=jax.ShapeDtypeStruct((copies, 16, LANES), F32),
        in_specs=[VMEM, VMEM],
        out_specs=VMEM,
        scratch_shapes=[
            pltpu.VMEM((PLANE * depth, (FULL + 1) * LANES), BF16),
            pltpu.VMEM((2 * YS * ROWS, (FULL + 1) * LANES), F32),
        ],
        compiler_params=pltpu.CompilerParams(vmem_limit_bytes=12 * MIB),
        name="score",
    )(rows, weights)


def merged(lse, cross, answer, clean_lse):
    top = jnp.max(lse, axis=0)
    lse = top + jnp.log(jnp.sum(jnp.exp(lse - top), axis=0))
    top = jnp.max(clean_lse, axis=0)
    weight = jnp.exp(clean_lse - top)
    total = jnp.sum(weight, axis=0)
    cross = jnp.sum(weight * cross, axis=0) / total
    return lse, cross, jnp.sum(answer, axis=0), top + jnp.log(total)


def merge_kernel(in_ref, layer_ref, pos_ref, out_ref, *, position_count):
    me = lax.axis_index("cells")
    y, core = (me // CORES) % YS, me % CORES
    lines = []
    for value in merged(*(in_ref[:, 4 * k : 4 * k + 4, :] for k in range(4))):
        value = jnp.where(core == 1, pltpu.roll(value, KEYS, 1), value)
        placed = value
        for shift in range(1, YS):
            turned = jnp.concatenate([value[YS - shift :], value[: YS - shift]], axis=0)
            placed = jnp.where(y == shift, turned, placed)
        lines.append(placed)
    hits = key_hits(layer_ref, pos_ref, position_count)
    count = as_line(jnp.sum(hits, axis=1, keepdims=True))
    lane = lanes_of((YS, LANES))
    row = lax.broadcasted_iota(jnp.int32, (YS, LANES), 0)
    half = KEYS // 2
    count = jnp.where(row == 0, pltpu.roll(count, half, 1), count)
    lines[3] = jnp.where((lane // half == 1) & (row < 2), count, lines[3])
    for i in range(out_ref.shape[0]):
        for k in range(4):
            out_ref[i, 4 * k : 4 * k + 4, :] = lines[k]


def merged_over_vocab(pieces, layer, pos, position_count):
    return pl.pallas_call(
        functools.partial(merge_kernel, position_count=position_count),
        out_shape=jax.ShapeDtypeStruct((PLANE, 16, LANES), F32),
        in_specs=[VMEM, VMEM, VMEM],
        out_specs=VMEM,
        compiler_params=pltpu.CompilerParams(vmem_limit_bytes=8 * MIB),
        name="merge",
    )(pieces, layer, pos)


def finish_kernel(in_ref, layer_ref, pos_ref, div_ref, log_ref, total_ref, *, position_count):
    me = lax.axis_index("cells")
    shape = (YS, LANES)
    row = lax.broadcasted_iota(jnp.int32, shape, 0)
    lane = lanes_of(shape)
    half = KEYS // 2
    own_row = (me // CORES) % YS
    total = jnp.zeros(shape, F32)
    own_div = jnp.zeros(shape, F32)
    own_log = jnp.zeros(shape, F32)
    for x in range(XS):
        group = slice(x * SUBS, (x + 1) * SUBS)
        clean = in_ref[group, 12:16, :]
        spread = [
            jnp.where(lane % KEYS < half, clean[s], pltpu.roll(clean[s], half, 1))[None]
            for s in range(SUBS)
        ]
        lse, cross, answer, clean_lse = merged(
            *(in_ref[group, 4 * k : 4 * k + 4, :] for k in range(3)),
            jnp.concatenate(spread, axis=0),
        )
        divergence = cross - clean_lse + lse
        for s in range(SUBS):
            y, core = s // CORES, s % CORES
            left = pltpu.roll(clean[s], (core * KEYS - half) % LANES, 1)[0:1]
            right = clean[s][1:2]
            if core == 1:
                right = pltpu.roll(clean[s], KEYS, 1)[1:2]
            count = jnp.where(lane[0:1] % KEYS < half, left, right)
            count = jnp.where(lane[0:1] // KEYS == core, count, 0.0)
            total = total + jnp.where(row == y, count * divergence, 0.0)
        mine = (row == own_row) & (me // SUBS == x)
        own_div = jnp.where(mine, divergence, own_div)
        own_log = jnp.where(mine, answer - lse, own_log)
    total_ref[...] = jnp.sum(jnp.sum(total, axis=0, keepdims=True), axis=1, keepdims=True)
    own = jnp.concatenate(
        [
            jnp.sum(own_div, axis=0, keepdims=True),
            jnp.sum(own_log, axis=0, keepdims=True),
            jnp.zeros((6, LANES), F32),
        ],
        axis=0,
    )
    own = jnp.where(me % CORES == 1, pltpu.roll(own, KEYS, 1), own)
    hits = key_hits(layer_ref, pos_ref, position_count)
    out = jnp.dot(own, hits, preferred_element_type=F32, precision=lax.Precision.HIGHEST)
    div_ref[...] = out[0]
    log_ref[...] = out[1]


def finished(pieces, layer, pos, position_count):
    cells = layer.shape[1]
    return pl.pallas_call(
        functools.partial(finish_kernel, position_count=position_count),
        out_shape=(
            jax.ShapeDtypeStruct((cells,), F32),
            jax.ShapeDtypeStruct((cells,), F32),
            jax.ShapeDtypeStruct((1, 1), F32),
        ),
        in_specs=[VMEM, VMEM, VMEM],
        out_specs=(VMEM, VMEM, VMEM),
        compiler_params=pltpu.CompilerParams(vmem_limit_bytes=8 * MIB),
        name="finish",
    )(pieces, layer, pos)


def moved(value, to):
    return lax.ppermute(value, "cells", [(i, to(i)) for i in range(PLANE)])


def along_y(step):
    def to(i):
        x, y, core = i // SUBS, (i // CORES) % YS, i % CORES
        return x * SUBS + ((y - step) % YS) * CORES + core

    return to


def on_device(clean_resid, path_delta, layer_index, pos_index, answer_ids, norm_gain, unembed):
    position_count = path_delta.shape[2]
    features = clean_resid.shape[1]
    act, sent = prepared(
        answer_ids,
        clean_resid,
        path_delta.reshape(KEYS, features),
        norm_gain.reshape(1, features),
        unembed,
    )
    same = [act]
    for step in range(1, YS):
        same.append(moved(act, along_y(step)))
    weights = lax.all_to_all(sent, "cells", 0, 0, tiled=True)
    other = []
    for step in range(YS):
        other.append(moved(same[step], lambda i: i ^ 1))
    stats = scored(stacked(same + other), weights, lax.axis_size("vocab"))
    stats = lax.all_to_all(stats, "vocab", 0, 0, tiled=True)
    layer, pos = layer_index.reshape(1, -1), pos_index.reshape(1, -1)
    pieces = merged_over_vocab(stats, layer, pos, position_count)
    pieces = lax.all_to_all(pieces, "cells", 0, 0, tiled=True)
    divergence, answer_logprob, total = finished(pieces, layer, pos, position_count)
    return divergence, answer_logprob, total.reshape(())


def solution(mesh):
    in_specs = (
        P("cells", None),
        P("cells", None, None, None),
        P("cells"),
        P("cells"),
        P("cells"),
        P(),
        P("cells", "vocab"),
    )
    out_specs = (P("cells"), P("cells"), P())
    return jax.shard_map(
        on_device, mesh=mesh, in_specs=in_specs, out_specs=out_specs, check_vma=False
    )
```

```python
import functools

import jax
import jax.numpy as jnp
from jax import lax
from jax.experimental import pallas as pl
from jax.experimental.pallas import tpu as pltpu
from jax.sharding import PartitionSpec as P


XS, YS, CORES = 4, 4, 2
SUBS = YS * CORES
PLANE = XS * SUBS
LANES = 128
KEYS = 64
ROWS = 72
FULL = 3
LEFT = LANES // SUBS
NEG = -1e30
CHUNKS = 4
F32 = jnp.float32
BF16 = jnp.bfloat16
MIB = 1 << 20
VMEM = pl.BlockSpec(memory_space=pltpu.VMEM)
SMEM = pl.BlockSpec(memory_space=pltpu.SMEM)


def lanes_of(shape):
    return lax.broadcasted_iota(jnp.int32, shape, len(shape) - 1)


def key_hits(layer_ref, pos_ref, position_count):
    flat = layer_ref[...] * position_count + pos_ref[...]
    key = lax.broadcasted_iota(jnp.int32, (LANES, flat.shape[1]), 0)
    return (key == flat).astype(F32)


def as_line(column):
    square = (LANES, LANES)
    eye = lax.broadcasted_iota(jnp.int32, square, 0) == lanes_of(square)
    return jnp.sum(jnp.where(eye, column, 0.0), axis=0, keepdims=True)


def pack_columns(u_ref, out_ref):
    depth = u_ref.shape[0]
    groups = depth // 8
    last = u_ref[:, SUBS * FULL * LANES :].astype(F32)
    lane = lanes_of((8, LANES))
    for sub in range(SUBS):
        left = jnp.zeros((8, LANES), F32)
        for a in range(groups):
            piece = pltpu.roll(last[8 * a : 8 * a + 8], (LEFT * (a - sub)) % LANES, 1)
            left = jnp.where(lane // LEFT == a, piece, left)
        left = left.astype(BF16)
        for x in range(XS):
            to = x * SUBS + sub
            for k in range(FULL):
                at = (sub * FULL + k) * LANES
                out_ref[to, k * depth : (k + 1) * depth, :] = u_ref[:, at : at + LANES]
            out_ref[to, FULL * depth :, :] = left


def norm_rows(answer_ref, clean_ref, delta_ref, gain_ref, act_ref):
    features = clean_ref.shape[1]
    clean = clean_ref[...]
    gain = gain_ref[...]

    def normed(values):
        mean_square = jnp.sum(values * values, axis=-1, keepdims=True) * (1.0 / features)
        return values * lax.rsqrt(mean_square + 1e-06) * gain

    act_ref[:KEYS, :] = normed(clean + delta_ref[...].astype(F32)).astype(BF16)
    answer = answer_ref[0]
    high = lax.shift_right_logical(answer, 8).astype(F32)
    low = (answer & 255).astype(F32)
    shape = (ROWS - KEYS, features)
    row = lax.broadcasted_iota(jnp.int32, shape, 0)
    lane = lanes_of(shape)
    digits = jnp.where(lane == 0, high, jnp.where(lane == 1, low, 0.0))
    tail = jnp.where(row == 0, normed(clean), jnp.where(row == 1, digits, 0.0))
    act_ref[KEYS:, :] = tail.astype(BF16)


def prepare_kernel(answer_ref, *refs):
    sources, (act_ref, pack_ref), buffers, sems = refs[:4], refs[4:6], refs[6:10], refs[10]
    copies = [
        pltpu.make_async_copy(source, buffer, sems.at[k])
        for k, (source, buffer) in enumerate(zip(sources, buffers))
    ]
    for copy in copies:
        copy.start()
    for copy in copies[:3]:
        copy.wait()
    clean, delta, gain, columns = buffers
    norm_rows(answer_ref, clean, delta, gain, act_ref)
    copies[3].wait()
    pack_columns(columns, pack_ref)


def prepared(answer_ids, clean_resid, delta_table, norm_gain, unembed):
    arrays = (clean_resid, delta_table, norm_gain, unembed)
    depth = unembed.shape[0]
    return pl.pallas_call(
        prepare_kernel,
        out_shape=(
            jax.ShapeDtypeStruct((ROWS, clean_resid.shape[1]), BF16),
            jax.ShapeDtypeStruct((PLANE, FULL * depth + 8, LANES), BF16),
        ),
        in_specs=[SMEM] + [pl.BlockSpec(memory_space=pltpu.HBM)] * 4,
        out_specs=(VMEM, VMEM),
        scratch_shapes=[pltpu.VMEM(array.shape, array.dtype) for array in arrays]
        + [pltpu.SemaphoreType.DMA((4,))],
        compiler_params=pltpu.CompilerParams(vmem_limit_bytes=67043328),
        name="prepare",
    )(answer_ids, *arrays)


def stack_kernel(*refs):
    acts, out_ref = refs[:SUBS], refs[SUBS]
    for j in range(SUBS):
        out_ref[j * ROWS : (j + 1) * ROWS, :] = acts[j][...]


def stacked(acts):
    return pl.pallas_call(
        stack_kernel,
        out_shape=jax.ShapeDtypeStruct((SUBS * ROWS, acts[0].shape[1]), BF16),
        in_specs=[VMEM] * SUBS,
        out_specs=VMEM,
        compiler_params=pltpu.CompilerParams(vmem_limit_bytes=8 * MIB),
        name="stack",
    )(*acts)


def score_kernel(a_ref, w_ref, out_ref, w_buf, t_buf, r_buf, l_buf, sems):
    depth = w_buf.shape[1]
    groups = depth // 8
    copies = out_ref.shape[0]
    me = lax.axis_index("cells")
    sub = me % SUBS
    start = lax.axis_index("vocab") * (SUBS * (FULL * LANES + LEFT))
    per = PLANE // CHUNKS
    moves = []
    for c in range(CHUNKS):
        blocks = pl.ds(c * per, per)
        pairs = [
            (
                w_ref.at[blocks, pl.ds(k * depth, depth), :],
                w_buf.at[blocks, :, pl.ds(k * LANES, LANES)],
            )
            for k in range(FULL)
        ]
        pairs.append((w_ref.at[blocks, pl.ds(FULL * depth, 8), :], t_buf.at[blocks]))
        moves.append(
            [
                pltpu.make_async_copy(source, target, sems.at[c * (FULL + 1) + k])
                for k, (source, target) in enumerate(pairs)
            ]
        )
    for move in moves:
        for copy in move:
            copy.start()
    for c in range(CHUNKS):
        for copy in moves[c]:
            copy.wait()
        blocks = slice(c * per, (c + 1) * per)
        for i in range(c * per, (c + 1) * per):
            left = t_buf[i].astype(F32)
            pieces = [left] + [pltpu.roll(left, LANES - LEFT * a, 1) for a in range(1, groups)]
            r_buf[i] = jnp.concatenate(pieces, axis=0).astype(BF16)
        features = per * depth
        columns = jnp.concatenate(
            [
                w_buf[blocks].reshape(features, FULL * LANES),
                r_buf[blocks].reshape(features, LANES),
            ],
            axis=1,
        )
        rows = a_ref[:, c * features : (c + 1) * features]
        part = jnp.dot(rows, columns, preferred_element_type=F32)
        l_buf[...] = part if c == 0 else l_buf[...] + part

    width = (FULL + 1) * LANES
    lane = lanes_of((1, width))
    kept = lane < FULL * LANES + LEFT
    column = jnp.where(
        lane < FULL * LANES,
        start + sub * (FULL * LANES) + lane,
        start + SUBS * FULL * LANES + sub * LEFT + lane - FULL * LANES,
    ).astype(F32)
    clean_line = jnp.zeros((1, LANES), F32)
    slot = lanes_of((1, LANES))
    for t in range(YS):
        parts = []
        for d in range(CORES):
            at = (d * YS + t) * ROWS
            clean = jnp.where(kept, l_buf[at + KEYS : at + KEYS + 1, :], NEG)
            max_clean = jnp.max(clean, axis=-1, keepdims=True)
            weight = jnp.exp(clean - max_clean)
            sum_clean = jnp.sum(weight, axis=-1, keepdims=True)
            weight = weight * (1.0 / sum_clean)
            clean_lse = max_clean + jnp.log(sum_clean)
            tail = a_ref[at + KEYS : at + ROWS, 0:LANES].astype(F32)
            digits = tail[1:2]
            answer = digits[:, 0:1] * 256.0 + digits[:, 1:2]
            logits = jnp.where(kept, l_buf[at : at + KEYS, :], NEG)
            max_patch = jnp.max(logits, axis=-1, keepdims=True)
            sum_patch = jnp.sum(jnp.exp(logits - max_patch), axis=-1, keepdims=True)
            cross = jnp.sum(weight * (clean - logits), axis=-1, keepdims=True)
            picked = jnp.where((column == answer) & kept, logits, 0.0)
            parts.append(
                (
                    max_patch + jnp.log(sum_patch),
                    cross,
                    jnp.sum(picked, axis=-1, keepdims=True),
                )
            )
            clean_line = jnp.where(slot == t * CORES + d, clean_lse, clean_line)
        for k in range(3):
            both = jnp.concatenate([parts[0][k], parts[1][k]], axis=0)
            line = as_line(both)
            for i in range(copies):
                out_ref[i, :, (4 * k + t) * LANES : (4 * k + t + 1) * LANES] = line
    for i in range(copies):
        out_ref[i, :, 12 * LANES :] = clean_line


def scored(rows, weights, copies):
    depth = (weights.shape[1] - 8) // FULL
    return pl.pallas_call(
        score_kernel,
        out_shape=jax.ShapeDtypeStruct((copies, 1, 13 * LANES), F32),
        in_specs=[VMEM, pl.BlockSpec(memory_space=pltpu.HBM)],
        out_specs=VMEM,
        scratch_shapes=[
            pltpu.VMEM((PLANE, depth, FULL * LANES), BF16),
            pltpu.VMEM((PLANE, 8, LANES), BF16),
            pltpu.VMEM((PLANE, depth, LANES), BF16),
            pltpu.VMEM((2 * YS * ROWS, (FULL + 1) * LANES), F32),
            pltpu.SemaphoreType.DMA((CHUNKS * (FULL + 1),)),
        ],
        compiler_params=pltpu.CompilerParams(vmem_limit_bytes=12 * MIB),
        name="score",
    )(rows, weights)


def merged(lse, cross, answer, clean_lse):
    top = jnp.max(lse, axis=0, keepdims=True)
    lse = top + jnp.log(jnp.sum(jnp.exp(lse - top), axis=0, keepdims=True))
    top = jnp.max(clean_lse, axis=0, keepdims=True)
    weight = jnp.exp(clean_lse - top)
    total = jnp.sum(weight, axis=0, keepdims=True)
    cross = jnp.sum(weight * cross, axis=0, keepdims=True) / total
    return lse, cross, jnp.sum(answer, axis=0, keepdims=True), top + jnp.log(total)


def merge_kernel(in_ref, layer_ref, pos_ref, out_ref, *, position_count):
    me = lax.axis_index("cells")
    y, core = (me // CORES) % YS, me % CORES
    lane = lanes_of((1, LANES))
    clean = in_ref[:, 0, 12 * LANES :]
    by_slot = []
    for t in range(YS):
        first, second = (clean[:, t * CORES + d : t * CORES + d + 1] for d in range(CORES))
        clean_lse = jnp.where(lane < KEYS, first, second)
        stats = merged(
            *(in_ref[:, 0, (4 * k + t) * LANES : (4 * k + t + 1) * LANES] for k in range(3)),
            clean_lse,
        )
        by_slot.append(
            [jnp.where(core == 1, pltpu.roll(value, KEYS, 1), value) for value in stats]
        )
    hits = key_hits(layer_ref, pos_ref, position_count)
    count = as_line(jnp.sum(hits, axis=1, keepdims=True))
    half = KEYS // 2
    lines = []
    for k in range(4):
        for t in range(YS):
            line = by_slot[t][k]
            for shift in range(1, YS):
                line = jnp.where(y == shift, by_slot[(t - shift) % YS][k], line)
            if k == 3 and t < 2:
                piece = pltpu.roll(count, half, 1) if t == 0 else count
                line = jnp.where(lane // half == 1, piece, line)
            lines.append(line)
    block = jnp.concatenate(lines, axis=0)
    for i in range(out_ref.shape[0]):
        out_ref[i] = block


def merged_over_vocab(pieces, layer, pos, position_count):
    return pl.pallas_call(
        functools.partial(merge_kernel, position_count=position_count),
        out_shape=jax.ShapeDtypeStruct((PLANE, 16, LANES), F32),
        in_specs=[VMEM, VMEM, VMEM],
        out_specs=VMEM,
        compiler_params=pltpu.CompilerParams(vmem_limit_bytes=8 * MIB),
        name="merge",
    )(pieces, layer, pos)


def finish_kernel(in_ref, layer_ref, pos_ref, div_ref, log_ref, total_ref, *, position_count):
    me = lax.axis_index("cells")
    shape = (YS, LANES)
    row = lax.broadcasted_iota(jnp.int32, shape, 0)
    lane = lanes_of(shape)
    half = KEYS // 2
    own_row = (me // CORES) % YS
    total = jnp.zeros(shape, F32)
    own_div = jnp.zeros(shape, F32)
    own_log = jnp.zeros(shape, F32)
    for x in range(XS):
        group = slice(x * SUBS, (x + 1) * SUBS)
        clean = in_ref[group, 12:16, :]
        spread = [
            jnp.where(lane % KEYS < half, clean[s], pltpu.roll(clean[s], half, 1))[None]
            for s in range(SUBS)
        ]
        lse, cross, answer, clean_lse = (
            value[0]
            for value in merged(
                *(in_ref[group, 4 * k : 4 * k + 4, :] for k in range(3)),
                jnp.concatenate(spread, axis=0),
            )
        )
        divergence = cross - clean_lse + lse
        for s in range(SUBS):
            y, core = s // CORES, s % CORES
            left = pltpu.roll(clean[s], (core * KEYS - half) % LANES, 1)[0:1]
            right = clean[s][1:2]
            if core == 1:
                right = pltpu.roll(clean[s], KEYS, 1)[1:2]
            count = jnp.where(lane[0:1] % KEYS < half, left, right)
            count = jnp.where(lane[0:1] // KEYS == core, count, 0.0)
            total = total + jnp.where(row == y, count * divergence, 0.0)
        mine = (row == own_row) & (me // SUBS == x)
        own_div = jnp.where(mine, divergence, own_div)
        own_log = jnp.where(mine, answer - lse, own_log)
    total_ref[...] = jnp.sum(jnp.sum(total, axis=0, keepdims=True), axis=1, keepdims=True)
    own = jnp.concatenate(
        [
            jnp.sum(own_div, axis=0, keepdims=True),
            jnp.sum(own_log, axis=0, keepdims=True),
            jnp.zeros((6, LANES), F32),
        ],
        axis=0,
    )
    own = jnp.where(me % CORES == 1, pltpu.roll(own, KEYS, 1), own)
    hits = key_hits(layer_ref, pos_ref, position_count)
    out = jnp.dot(own, hits, preferred_element_type=F32, precision=lax.Precision.HIGHEST)
    div_ref[...] = out[0]
    log_ref[...] = out[1]


def finished(pieces, layer, pos, position_count):
    cells = layer.shape[1]
    return pl.pallas_call(
        functools.partial(finish_kernel, position_count=position_count),
        out_shape=(
            jax.ShapeDtypeStruct((cells,), F32),
            jax.ShapeDtypeStruct((cells,), F32),
            jax.ShapeDtypeStruct((1, 1), F32),
        ),
        in_specs=[VMEM, VMEM, VMEM],
        out_specs=(VMEM, VMEM, VMEM),
        compiler_params=pltpu.CompilerParams(vmem_limit_bytes=8 * MIB),
        name="finish",
    )(pieces, layer, pos)


def moved(value, to):
    return lax.ppermute(value, "cells", [(i, to(i)) for i in range(PLANE)])


def along_y(step):
    def to(i):
        x, y, core = i // SUBS, (i // CORES) % YS, i % CORES
        return x * SUBS + ((y - step) % YS) * CORES + core

    return to


def on_device(clean_resid, path_delta, layer_index, pos_index, answer_ids, norm_gain, unembed):
    position_count = path_delta.shape[2]
    features = clean_resid.shape[1]
    act, sent = prepared(
        answer_ids,
        clean_resid,
        path_delta.reshape(KEYS, features),
        norm_gain.reshape(1, features),
        unembed,
    )
    same = [act]
    for step in range(1, YS):
        same.append(moved(act, along_y(step)))
    weights = lax.all_to_all(sent, "cells", 0, 0, tiled=True)
    other = []
    for step in range(YS):
        other.append(moved(same[step], lambda i: i ^ 1))
    stats = scored(stacked(same + other), weights, lax.axis_size("vocab"))
    stats = lax.all_to_all(stats, "vocab", 0, 0, tiled=True)
    layer, pos = layer_index.reshape(1, -1), pos_index.reshape(1, -1)
    pieces = merged_over_vocab(stats, layer, pos, position_count)
    pieces = lax.all_to_all(pieces, "cells", 0, 0, tiled=True)
    divergence, answer_logprob, total = finished(pieces, layer, pos, position_count)
    return divergence, answer_logprob, total.reshape(())


def solution(mesh):
    in_specs = (
        P("cells", None),
        P("cells", None, None, None),
        P("cells"),
        P("cells"),
        P("cells"),
        P(),
        P("cells", "vocab"),
    )
    out_specs = (P("cells"), P("cells"), P())
    return jax.shard_map(
        on_device, mesh=mesh, in_specs=in_specs, out_specs=out_specs, check_vma=False
    )
```

```python
import functools

import jax
import jax.numpy as jnp
from jax import lax
from jax.experimental import pallas as pl
from jax.experimental.pallas import tpu as pltpu
from jax.sharding import PartitionSpec as P


XS, YS, CORES = 4, 4, 2
SUBS = YS * CORES
PLANE = XS * SUBS
LANES = 128
KEYS = 64
USED = SUBS * KEYS + 16
FULL = 3
LEFT = LANES // SUBS
NEG = -1e30
CHUNKS = 2
F32 = jnp.float32
BF16 = jnp.bfloat16
MIB = 1 << 20
VMEM = pl.BlockSpec(memory_space=pltpu.VMEM)
SMEM = pl.BlockSpec(memory_space=pltpu.SMEM)


def lanes_of(shape):
    return lax.broadcasted_iota(jnp.int32, shape, len(shape) - 1)


def key_hits(layer_ref, pos_ref, position_count):
    flat = layer_ref[...] * position_count + pos_ref[...]
    key = lax.broadcasted_iota(jnp.int32, (LANES, flat.shape[1]), 0)
    return (key == flat).astype(F32)


def as_line(column):
    square = (LANES, LANES)
    eye = lax.broadcasted_iota(jnp.int32, square, 0) == lanes_of(square)
    return jnp.sum(jnp.where(eye, column, 0.0), axis=0, keepdims=True)


def pack_columns(u_ref, out_ref):
    depth = u_ref.shape[0]
    groups = depth // 8
    last = u_ref[:, SUBS * FULL * LANES :].astype(F32)
    lane = lanes_of((8, LANES))
    for sub in range(SUBS):
        left = jnp.zeros((8, LANES), F32)
        for a in range(groups):
            piece = pltpu.roll(last[8 * a : 8 * a + 8], (LEFT * (a - sub)) % LANES, 1)
            left = jnp.where(lane // LEFT == a, piece, left)
        left = left.astype(BF16)
        for x in range(XS):
            to = x * SUBS + sub
            for k in range(FULL):
                at = (sub * FULL + k) * LANES
                out_ref[to, k * depth : (k + 1) * depth, :] = u_ref[:, at : at + LANES]
            out_ref[to, FULL * depth :, :] = left


def norm_rows(answer_ref, clean_ref, delta_ref, gain_ref, act_ref):
    features = clean_ref.shape[1]
    clean = clean_ref[...]
    gain = gain_ref[...]

    def normed(values):
        mean_square = jnp.sum(values * values, axis=-1, keepdims=True) * (1.0 / features)
        return values * lax.rsqrt(mean_square + 1e-06) * gain

    tiles = features // LANES
    patched = normed(clean + delta_ref[...].astype(F32)).astype(BF16)
    for k in range(tiles):
        act_ref[k * KEYS : (k + 1) * KEYS, :] = patched[:, k * LANES : (k + 1) * LANES]
    answer = answer_ref[0]
    high = lax.shift_right_logical(answer, 8).astype(F32)
    low = (answer & 255).astype(F32)
    clean_row = normed(clean)
    lines = [clean_row[:, k * LANES : (k + 1) * LANES] for k in range(tiles)]
    row = lax.broadcasted_iota(jnp.int32, (8, LANES), 0)
    lane = lanes_of((8, LANES))
    digits = jnp.where(lane == 0, high, jnp.where(lane == 1, low, 0.0))
    lines.append(jnp.where(row == 0, digits, 0.0))
    act_ref[tiles * KEYS :, :] = jnp.concatenate(lines, axis=0).astype(BF16)


def prepare_kernel(answer_ref, *refs):
    sources, (act_ref, pack_ref), buffers, sems = refs[:4], refs[4:6], refs[6:10], refs[10]
    copies = [
        pltpu.make_async_copy(source, buffer, sems.at[k])
        for k, (source, buffer) in enumerate(zip(sources, buffers))
    ]
    for copy in copies:
        copy.start()
    for copy in copies[:3]:
        copy.wait()
    clean, delta, gain, columns = buffers
    norm_rows(answer_ref, clean, delta, gain, act_ref)
    copies[3].wait()
    pack_columns(columns, pack_ref)


def prepared(answer_ids, clean_resid, delta_table, norm_gain, unembed):
    arrays = (clean_resid, delta_table, norm_gain, unembed)
    tiles = clean_resid.shape[1] // LANES
    depth = unembed.shape[0]
    return pl.pallas_call(
        prepare_kernel,
        out_shape=(
            jax.ShapeDtypeStruct((tiles * (KEYS + 1) + 8, LANES), BF16),
            jax.ShapeDtypeStruct((PLANE, FULL * depth + 8, LANES), BF16),
        ),
        in_specs=[SMEM] + [pl.BlockSpec(memory_space=pltpu.HBM)] * 4,
        out_specs=(VMEM, VMEM),
        scratch_shapes=[pltpu.VMEM(array.shape, array.dtype) for array in arrays]
        + [pltpu.SemaphoreType.DMA((4,))],
        compiler_params=pltpu.CompilerParams(vmem_limit_bytes=67043328),
        name="prepare",
    )(answer_ids, *arrays)


def stack_kernel(*refs):
    acts, out_ref = refs[:SUBS], refs[SUBS]
    tiles = out_ref.shape[1] // LANES
    for j in range(SUBS):
        for k in range(tiles):
            out_ref[j * KEYS : (j + 1) * KEYS, k * LANES : (k + 1) * LANES] = acts[j][
                k * KEYS : (k + 1) * KEYS, :
            ]
    tails = [acts[j][tiles * KEYS :, :].astype(F32) for j in range(SUBS)]
    digits = jnp.concatenate([tail[tiles : tiles + 1] for tail in tails], axis=0)
    for k in range(tiles):
        lines = [tail[k : k + 1] for tail in tails]
        spare = digits if k == 0 else jnp.zeros((SUBS, LANES), F32)
        block = jnp.concatenate(lines + [spare], axis=0).astype(BF16)
        out_ref[SUBS * KEYS : USED, k * LANES : (k + 1) * LANES] = block


def stacked(acts):
    tiles = acts[0].shape[0] // (KEYS + 1)
    return pl.pallas_call(
        stack_kernel,
        out_shape=jax.ShapeDtypeStruct((SUBS * (KEYS + 8), tiles * LANES), BF16),
        in_specs=[VMEM] * SUBS,
        out_specs=VMEM,
        compiler_params=pltpu.CompilerParams(vmem_limit_bytes=8 * MIB),
        name="stack",
    )(*acts)


def score_kernel(a_ref, w_ref, out_ref, w_buf, t_buf, r_buf, l_buf, sems):
    depth = w_buf.shape[1]
    groups = depth // 8
    copies = out_ref.shape[0]
    me = lax.axis_index("cells")
    sub = me % SUBS
    start = lax.axis_index("vocab") * (SUBS * (FULL * LANES + LEFT))
    per = PLANE // CHUNKS
    moves = []
    for c in range(CHUNKS):
        blocks = pl.ds(c * per, per)
        pairs = [
            (
                w_ref.at[blocks, pl.ds(k * depth, depth), :],
                w_buf.at[blocks, :, pl.ds(k * LANES, LANES)],
            )
            for k in range(FULL)
        ]
        pairs.append((w_ref.at[blocks, pl.ds(FULL * depth, 8), :], t_buf.at[blocks]))
        moves.append(
            [
                pltpu.make_async_copy(source, target, sems.at[c * (FULL + 1) + k])
                for k, (source, target) in enumerate(pairs)
            ]
        )
    for move in moves:
        for copy in move:
            copy.start()
    for c in range(CHUNKS):
        for copy in moves[c]:
            copy.wait()
        blocks = slice(c * per, (c + 1) * per)
        for i in range(c * per, (c + 1) * per):
            left = t_buf[i].astype(F32)
            pieces = [left] + [pltpu.roll(left, LANES - LEFT * a, 1) for a in range(1, groups)]
            r_buf[i] = jnp.concatenate(pieces, axis=0).astype(BF16)
        features = per * depth
        columns = jnp.concatenate(
            [
                w_buf[blocks].reshape(features, FULL * LANES),
                r_buf[blocks].reshape(features, LANES),
            ],
            axis=1,
        )
        rows = a_ref[:USED, c * features : (c + 1) * features]
        part = jnp.dot(rows, columns, preferred_element_type=F32)
        part = part if c == 0 else l_buf[...] + part
        if c < CHUNKS - 1:
            l_buf[...] = part
    l_buf[:, : FULL * LANES] = part[:, : FULL * LANES]
    last = part[:, FULL * LANES :]
    l_buf[:, FULL * LANES :] = jnp.where(lanes_of(last.shape) < LEFT, last, NEG)

    width = (FULL + 1) * LANES
    lane = lanes_of((1, width))
    kept = lane < FULL * LANES + LEFT
    column = jnp.where(
        lane < FULL * LANES,
        start + sub * (FULL * LANES) + lane,
        start + SUBS * FULL * LANES + sub * LEFT + lane - FULL * LANES,
    ).astype(F32)
    tail = a_ref[SUBS * KEYS : USED, 0:LANES].astype(F32)
    clean_line = jnp.zeros((1, LANES), F32)
    slot = lanes_of((1, LANES))
    for t in range(YS):
        parts = []
        for d in range(CORES):
            j = d * YS + t
            clean = l_buf[SUBS * KEYS + j : SUBS * KEYS + j + 1, :]
            max_clean = jnp.max(clean, axis=-1, keepdims=True)
            weight = jnp.exp(clean - max_clean)
            sum_clean = jnp.sum(weight, axis=-1, keepdims=True)
            weight = weight * (1.0 / sum_clean)
            clean_lse = max_clean + jnp.log(sum_clean)
            digits = tail[SUBS + j : SUBS + j + 1]
            answer = digits[:, 0:1] * 256.0 + digits[:, 1:2]
            logits = l_buf[j * KEYS : (j + 1) * KEYS, :]
            max_patch = jnp.max(logits, axis=-1, keepdims=True)
            sum_patch = jnp.sum(jnp.exp(logits - max_patch), axis=-1, keepdims=True)
            cross = jnp.sum(weight * (clean - logits), axis=-1, keepdims=True)
            picked = jnp.where((column == answer) & kept, logits, 0.0)
            parts.append(
                (
                    max_patch + jnp.log(sum_patch),
                    cross,
                    jnp.sum(picked, axis=-1, keepdims=True),
                )
            )
            clean_line = jnp.where(slot == t * CORES + d, clean_lse, clean_line)
        for k in range(3):
            both = jnp.concatenate([parts[0][k], parts[1][k]], axis=0)
            line = as_line(both)
            for i in range(copies):
                out_ref[i, :, (4 * k + t) * LANES : (4 * k + t + 1) * LANES] = line
    for i in range(copies):
        out_ref[i, :, 12 * LANES :] = clean_line


def scored(rows, weights, copies):
    depth = (weights.shape[1] - 8) // FULL
    return pl.pallas_call(
        score_kernel,
        out_shape=jax.ShapeDtypeStruct((copies, 1, 13 * LANES), F32),
        in_specs=[VMEM, pl.BlockSpec(memory_space=pltpu.HBM)],
        out_specs=VMEM,
        scratch_shapes=[
            pltpu.VMEM((PLANE, depth, FULL * LANES), BF16),
            pltpu.VMEM((PLANE, 8, LANES), BF16),
            pltpu.VMEM((PLANE, depth, LANES), BF16),
            pltpu.VMEM((USED, (FULL + 1) * LANES), F32),
            pltpu.SemaphoreType.DMA((CHUNKS * (FULL + 1),)),
        ],
        compiler_params=pltpu.CompilerParams(vmem_limit_bytes=12 * MIB),
        name="score",
    )(rows, weights)


def merged(lse, cross, answer, clean_lse):
    top = jnp.max(lse, axis=0, keepdims=True)
    lse = top + jnp.log(jnp.sum(jnp.exp(lse - top), axis=0, keepdims=True))
    top = jnp.max(clean_lse, axis=0, keepdims=True)
    weight = jnp.exp(clean_lse - top)
    total = jnp.sum(weight, axis=0, keepdims=True)
    cross = jnp.sum(weight * cross, axis=0, keepdims=True) / total
    return lse, cross, jnp.sum(answer, axis=0, keepdims=True), top + jnp.log(total)


def merge_kernel(in_ref, layer_ref, pos_ref, out_ref, *, position_count):
    me = lax.axis_index("cells")
    y, core = (me // CORES) % YS, me % CORES
    lane = lanes_of((1, LANES))
    clean = in_ref[:, 0, 12 * LANES :]
    by_slot = []
    for t in range(YS):
        first, second = (clean[:, t * CORES + d : t * CORES + d + 1] for d in range(CORES))
        clean_lse = jnp.where(lane < KEYS, first, second)
        stats = merged(
            *(in_ref[:, 0, (4 * k + t) * LANES : (4 * k + t + 1) * LANES] for k in range(3)),
            clean_lse,
        )
        by_slot.append(
            [jnp.where(core == 1, pltpu.roll(value, KEYS, 1), value) for value in stats]
        )
    hits = key_hits(layer_ref, pos_ref, position_count)
    count = as_line(jnp.sum(hits, axis=1, keepdims=True))
    half = KEYS // 2
    lines = []
    for k in range(4):
        for t in range(YS):
            line = by_slot[t][k]
            for shift in range(1, YS):
                line = jnp.where(y == shift, by_slot[(t - shift) % YS][k], line)
            if k == 3 and t < 2:
                piece = pltpu.roll(count, half, 1) if t == 0 else count
                line = jnp.where(lane // half == 1, piece, line)
            lines.append(line)
    block = jnp.concatenate(lines, axis=0)
    for i in range(out_ref.shape[0]):
        out_ref[i] = block


def merged_over_vocab(pieces, layer, pos, position_count):
    return pl.pallas_call(
        functools.partial(merge_kernel, position_count=position_count),
        out_shape=jax.ShapeDtypeStruct((PLANE, 16, LANES), F32),
        in_specs=[VMEM, VMEM, VMEM],
        out_specs=VMEM,
        compiler_params=pltpu.CompilerParams(vmem_limit_bytes=8 * MIB),
        name="merge",
    )(pieces, layer, pos)


def finish_kernel(in_ref, layer_ref, pos_ref, div_ref, log_ref, total_ref, *, position_count):
    me = lax.axis_index("cells")
    shape = (YS, LANES)
    row = lax.broadcasted_iota(jnp.int32, shape, 0)
    lane = lanes_of(shape)
    half = KEYS // 2
    own_row = (me // CORES) % YS
    total = jnp.zeros(shape, F32)
    own_div = jnp.zeros(shape, F32)
    own_log = jnp.zeros(shape, F32)
    for x in range(XS):
        group = slice(x * SUBS, (x + 1) * SUBS)
        clean = in_ref[group, 12:16, :]
        spread = [
            jnp.where(lane % KEYS < half, clean[s], pltpu.roll(clean[s], half, 1))[None]
            for s in range(SUBS)
        ]
        lse, cross, answer, clean_lse = (
            value[0]
            for value in merged(
                *(in_ref[group, 4 * k : 4 * k + 4, :] for k in range(3)),
                jnp.concatenate(spread, axis=0),
            )
        )
        divergence = cross - clean_lse + lse
        for s in range(SUBS):
            y, core = s // CORES, s % CORES
            left = pltpu.roll(clean[s], (core * KEYS - half) % LANES, 1)[0:1]
            right = clean[s][1:2]
            if core == 1:
                right = pltpu.roll(clean[s], KEYS, 1)[1:2]
            count = jnp.where(lane[0:1] % KEYS < half, left, right)
            count = jnp.where(lane[0:1] // KEYS == core, count, 0.0)
            total = total + jnp.where(row == y, count * divergence, 0.0)
        mine = (row == own_row) & (me // SUBS == x)
        own_div = jnp.where(mine, divergence, own_div)
        own_log = jnp.where(mine, answer - lse, own_log)
    total_ref[...] = jnp.sum(jnp.sum(total, axis=0, keepdims=True), axis=1, keepdims=True)
    own = jnp.concatenate(
        [
            jnp.sum(own_div, axis=0, keepdims=True),
            jnp.sum(own_log, axis=0, keepdims=True),
            jnp.zeros((6, LANES), F32),
        ],
        axis=0,
    )
    own = jnp.where(me % CORES == 1, pltpu.roll(own, KEYS, 1), own)
    hits = key_hits(layer_ref, pos_ref, position_count)
    out = jnp.dot(own, hits, preferred_element_type=F32, precision=lax.Precision.HIGHEST)
    div_ref[...] = out[0]
    log_ref[...] = out[1]


def finished(pieces, layer, pos, position_count):
    cells = layer.shape[1]
    return pl.pallas_call(
        functools.partial(finish_kernel, position_count=position_count),
        out_shape=(
            jax.ShapeDtypeStruct((cells,), F32),
            jax.ShapeDtypeStruct((cells,), F32),
            jax.ShapeDtypeStruct((1, 1), F32),
        ),
        in_specs=[VMEM, VMEM, VMEM],
        out_specs=(VMEM, VMEM, VMEM),
        compiler_params=pltpu.CompilerParams(vmem_limit_bytes=8 * MIB),
        name="finish",
    )(pieces, layer, pos)


def moved(value, to):
    return lax.ppermute(value, "cells", [(i, to(i)) for i in range(PLANE)])


def along_y(step):
    def to(i):
        x, y, core = i // SUBS, (i // CORES) % YS, i % CORES
        return x * SUBS + ((y - step) % YS) * CORES + core

    return to


def on_device(clean_resid, path_delta, layer_index, pos_index, answer_ids, norm_gain, unembed):
    position_count = path_delta.shape[2]
    features = clean_resid.shape[1]
    act, sent = prepared(
        answer_ids,
        clean_resid,
        path_delta.reshape(KEYS, features),
        norm_gain.reshape(1, features),
        unembed,
    )
    same = [act]
    for step in range(1, YS):
        same.append(moved(act, along_y(step)))
    weights = lax.all_to_all(sent, "cells", 0, 0, tiled=True)
    other = []
    for step in range(YS):
        other.append(moved(same[step], lambda i: i ^ 1))
    stats = scored(stacked(same + other), weights, lax.axis_size("vocab"))
    stats = lax.all_to_all(stats, "vocab", 0, 0, tiled=True)
    layer, pos = layer_index.reshape(1, -1), pos_index.reshape(1, -1)
    pieces = merged_over_vocab(stats, layer, pos, position_count)
    pieces = lax.all_to_all(pieces, "cells", 0, 0, tiled=True)
    divergence, answer_logprob, total = finished(pieces, layer, pos, position_count)
    return divergence, answer_logprob, total.reshape(())


def solution(mesh):
    in_specs = (
        P("cells", None),
        P("cells", None, None, None),
        P("cells"),
        P("cells"),
        P("cells"),
        P(),
        P("cells", "vocab"),
    )
    out_specs = (P("cells"), P("cells"), P())
    return jax.shard_map(
        on_device, mesh=mesh, in_specs=in_specs, out_specs=out_specs, check_vma=False
    )
```
